32 devices in a mesh: seg: 4 (over z), ch: 8 (over y, x, core).
Axes of the slice: x: 2, y: 2, z: 4, core: 2. Of those that a mesh axis runs over, the one named last changes fastest.
Arguments:
- gate_in: bfloat16 [1536, 16384], P('ch', 'seg'), may hold values from -6 to 6
- key_in: bfloat16 [1536, 16384], P('ch', 'seg'), may hold values from -6 to 6
- value_in: bfloat16 [1536, 16384], P('ch', 'seg'), may hold values from -6 to 6
- kernel: float32 [1536, 16384], P('ch'), may hold values from -0.046875 to 0.046875
- skip_gain: float32 [1536], P('ch'), may hold values from -1 to 1
- out_weight: bfloat16 [1536, 1536], P('ch'), may hold values from -0.15625 to 0.15625
Outputs:
- output: bfloat16 [16384, 1536], P(('seg', 'ch'))
The draws below stay inside these ranges and needn't reach their ends.
All inputs are finite; a program needn't handle non-finite values.
Results may differ from the reference program's by a relative error of at most 0.0095.
Values may be sent and summed in bfloat16 or wider, within the bound.
A program may use at most 128 MiB of HBM per device.

```python
import jax
import jax.numpy as jnp
from jax import lax

D = 1536
SEQ = 16384


def level_of(rng, extent, cuts, least, top_value):
    level = 1.0
    for axis_at, shards_of in cuts:
        heights = jax.random.uniform(jax.random.fold_in(jax.random.fold_in(rng, 6), axis_at), (shards_of,), jnp.float32, least / len(cuts), top_value / len(cuts))
        level = level * jnp.repeat(jnp.exp(heights), extent[axis_at] // shards_of).reshape((-1,) + (1,) * (len(extent) - 1 - axis_at))
    return level


def bell_draw(key, extent, deviation, bound, split=(), dtype=jnp.bfloat16):
    drawn = deviation * jax.random.normal(key, extent, jnp.float32)
    if split:
        drawn = drawn * level_of(key, extent, split, -0.22, 0.18)
    return jnp.clip(drawn, -bound, bound).astype(dtype)


def setup_inputs(seed: int = 0) -> dict:
    key_list = jax.random.split(jax.random.key(seed), 7)
    gate_in = bell_draw(key_list[0], (D, SEQ), 1.0, 6.0, ((0, 8), (1, 4)))
    key_in = bell_draw(key_list[1], (D, SEQ), 1.0, 6.0, ((0, 8), (1, 4)))
    value_in = bell_draw(key_list[2], (D, SEQ), 1.0, 6.0, ((0, 8), (1, 4)))
    kernel = bell_draw(key_list[3], (D, SEQ), SEQ ** -0.5, 0.046875, ((0, 8),), jnp.float32)
    skip_gain = jnp.clip(jax.random.uniform(key_list[4], (D,), jnp.float32, -1.0, 1.0) * level_of(key_list[4], (D,), ((0, 8),), -0.4, 0.0), -1.0, 1.0)
    out_weight = bell_draw(key_list[5], (D, D), D ** -0.5, 0.15625, ((0, 8),))
    return dict(gate_in=gate_in, key_in=key_in, value_in=value_in, kernel=kernel, skip_gain=skip_gain, out_weight=out_weight)


def reference(gate_in, key_in, value_in, kernel, skip_gain, out_weight):
    mixed_in = key_in.astype(jnp.float32) * value_in.astype(jnp.float32)
    length = mixed_in.shape[1]
    product = jnp.fft.rfft(mixed_in, n=2 * length, axis=1) * jnp.fft.rfft(kernel, n=2 * length, axis=1)
    convolved = jnp.fft.irfft(product, n=2 * length, axis=1)[:, :length]
    gated = (gate_in.astype(jnp.float32) * (convolved + skip_gain[:, None] * mixed_in)).astype(jnp.bfloat16)
    result = lax.dot_general(gated, out_weight, (((0,), (0,)), ((), ())), preferred_element_type=jnp.float32)
    return result.astype(jnp.bfloat16)
```

```python
import functools
import math

import jax
import jax.numpy as jnp
from jax import lax
from jax.experimental import pallas as pl
from jax.experimental.pallas import tpu as pltpu
from jax.sharding import PartitionSpec as P

lane_width = 128
bf16 = jnp.bfloat16
f32 = jnp.float32


def angles(rows, cols, period):
    product = rows[:, None] * cols[None, :] % (4 * period)
    theta = product.astype(f32) * (2.0 * math.pi / (4 * period))
    return jnp.cos(theta), jnp.sin(theta)


def make_tables(outer):
    quarter = 4 * jnp.arange(outer, dtype=jnp.int32) + 1
    row = jnp.arange(outer, dtype=jnp.int32)
    lane = jnp.arange(lane_width, dtype=jnp.int32)
    cos_o, sin_o = angles(quarter, row, outer)
    cos_t, sin_t = angles(quarter, lane, outer * lane_width)
    cos_i, sin_i = angles(4 * lane, lane, lane_width)
    first = jnp.concatenate([cos_o, -sin_o], axis=0).astype(bf16)
    last = (jnp.concatenate([cos_o.T, -sin_o.T], axis=1) / (outer * lane_width)).astype(bf16)
    inner = jnp.block([[cos_i, -sin_i], [sin_i, cos_i]]).astype(bf16)
    inner_back = jnp.block([[cos_i, sin_i], [-sin_i, cos_i]]).astype(bf16)
    return first, last, inner, inner_back, cos_t, sin_t


def forward(signal, first, inner, cos_t, sin_t):
    outer = cos_t.shape[0]
    rows = []
    for at in range(0, len(signal), 2):
        pair = signal[at : at + 2]
        wide = jnp.dot(first, jnp.concatenate(pair, axis=1), preferred_element_type=f32)
        for i in range(len(pair)):
            part = wide[:, i * lane_width : (i + 1) * lane_width]
            real, imag = part[:outer], part[outer:]
            rows.append(
                jnp.concatenate(
                    [
                        (real * cos_t + imag * sin_t).astype(bf16),
                        (imag * cos_t - real * sin_t).astype(bf16),
                    ],
                    axis=1,
                )
            )
    return jnp.dot(jnp.concatenate(rows, axis=0), inner, preferred_element_type=f32)


def filter_kernel(first, inner, cos_t, sin_t, taps, spectrum):
    count, outer = taps.shape[0], taps.shape[1]
    signal = [taps[i].astype(bf16) for i in range(count)]
    out = forward(signal, first[...], inner[...], cos_t[...], sin_t[...])
    spectrum[...] = out.astype(bf16).reshape(count, outer, 2 * lane_width)


def conv_kernel(first, last, inner, inner_back, cos_t, sin_t, mixed, spectrum, conv):
    count, outer = mixed.shape[0], mixed.shape[1]
    cos, sin = cos_t[...], sin_t[...]
    sig = forward([mixed[i] for i in range(count)], first[...], inner[...], cos, sin)
    filt = spectrum[...].reshape(count * outer, 2 * lane_width).astype(f32)
    sig_re, sig_im = sig[:, :lane_width], sig[:, lane_width:]
    filt_re, filt_im = filt[:, :lane_width], filt[:, lane_width:]
    prod = jnp.concatenate(
        [
            (filt_re * sig_re - filt_im * sig_im).astype(bf16),
            (filt_re * sig_im + filt_im * sig_re).astype(bf16),
        ],
        axis=1,
    )
    back = jnp.dot(prod, inner_back[...], preferred_element_type=f32)
    for at in range(0, count, 2):
        cols = []
        for i in range(at, min(at + 2, count)):
            rows = back[i * outer : (i + 1) * outer]
            real, imag = rows[:, :lane_width], rows[:, lane_width:]
            cols.append(
                jnp.concatenate(
                    [
                        (real * cos - imag * sin).astype(bf16),
                        (imag * cos + real * sin).astype(bf16),
                    ],
                    axis=0,
                )
            )
        wide = jnp.dot(last[...], jnp.concatenate(cols, axis=1), preferred_element_type=f32)
        for i in range(len(cols)):
            conv[at + i] = wide[:, i * lane_width : (i + 1) * lane_width].astype(bf16)


def whole(array):
    return pl.BlockSpec(array.shape, lambda i: (0,) * array.ndim)


def block_of(count):
    return max(b for b in range(1, 9) if count % b == 0)


def transform_filter(tables, taps):
    first, last, inner, inner_back, cos_t, sin_t = tables
    count, outer, lanes = taps.shape
    block = block_of(count)
    fixed = (first, inner, cos_t, sin_t)
    return pl.pallas_call(
        filter_kernel,
        grid=(count // block,),
        in_specs=[whole(a) for a in fixed] + [pl.BlockSpec((block, outer, lanes), lambda i: (i, 0, 0))],
        out_specs=pl.BlockSpec((block, outer, 2 * lanes), lambda i: (i, 0, 0)),
        out_shape=jax.ShapeDtypeStruct((count, outer, 2 * lanes), bf16),
        cost_estimate=pl.CostEstimate(
            flops=count * outer * lanes * 1536, bytes_accessed=count * outer * lanes * 8, transcendentals=0
        ),
        name="filter_transform",
    )(*fixed, taps)


def convolve(tables, mixed, spectrum):
    count, outer, lanes = mixed.shape
    block = block_of(count)
    return pl.pallas_call(
        conv_kernel,
        grid=(count // block,),
        in_specs=[whole(a) for a in tables]
        + [
            pl.BlockSpec((block, outer, lanes), lambda i: (i, 0, 0)),
            pl.BlockSpec((block, outer, 2 * lanes), lambda i: (i, 0, 0)),
        ],
        out_specs=pl.BlockSpec((block, outer, lanes), lambda i: (i, 0, 0)),
        out_shape=jax.ShapeDtypeStruct((count, outer, lanes), bf16),
        cost_estimate=pl.CostEstimate(
            flops=count * outer * lanes * 3072, bytes_accessed=count * outer * lanes * 8, transcendentals=0
        ),
        name="convolve",
    )(*tables, mixed, spectrum)


def on_device(gate_in, key_in, value_in, kernel, skip_gain, out_weight):
    seg_count = lax.axis_size("seg")
    seg_index = lax.axis_index("seg")
    channels, tokens = key_in.shape
    full_len = kernel.shape[1]
    outer = full_len // lane_width
    tables = make_tables(outer)
    col_count = channels // seg_count
    mixed = key_in.astype(f32) * value_in.astype(f32)
    mixed_sent = mixed.astype(bf16).reshape(channels, tokens // lane_width, lane_width)
    col_mixed = lax.all_to_all(mixed_sent, "seg", split_axis=0, concat_axis=1, tiled=True)
    taps = lax.dynamic_slice_in_dim(kernel, seg_index * col_count, col_count, 0)
    spectrum = transform_filter(tables, taps.astype(bf16).reshape(col_count, outer, lane_width))
    col_conv = convolve(tables, col_mixed, spectrum)
    conv = lax.all_to_all(col_conv, "seg", split_axis=1, concat_axis=0, tiled=True)
    conv = conv.reshape(channels, tokens).astype(f32)
    gated = (gate_in.astype(f32) * (conv + skip_gain[:, None] * mixed)).astype(bf16)
    mine = lax.all_to_all(gated, "ch", split_axis=1, concat_axis=0, tiled=True)
    weight = lax.all_gather(out_weight, "ch", axis=0, tiled=True)
    result = lax.dot_general(
        mine, weight, (((0,), (0,)), ((), ())), preferred_element_type=f32
    )
    return result.astype(bf16)


def solution(mesh):
    placed = (P("ch", "seg"), P("ch", "seg"), P("ch", "seg"), P("ch", None), P("ch"), P("ch", None))
    return jax.shard_map(
        on_device, mesh=mesh, in_specs=placed, out_specs=P(("seg", "ch"), None), check_vma=False
    )
```

```python
import functools
import math

import jax
import jax.numpy as jnp
from jax import lax
from jax.experimental import pallas as pl
from jax.experimental.pallas import tpu as pltpu
from jax.sharding import PartitionSpec as P

lane_width = 128
bf16 = jnp.bfloat16
f32 = jnp.float32


def angles(rows, cols, period):
    product = rows[:, None] * cols[None, :] % (4 * period)
    theta = product.astype(f32) * (2.0 * math.pi / (4 * period))
    return jnp.cos(theta), jnp.sin(theta)


def make_tables(outer):
    quarter = 4 * jnp.arange(outer, dtype=jnp.int32) + 1
    row = jnp.arange(outer, dtype=jnp.int32)
    lane = jnp.arange(lane_width, dtype=jnp.int32)
    cos_o, sin_o = angles(quarter, row, outer)
    cos_t, sin_t = angles(quarter, lane, outer * lane_width)
    cos_i, sin_i = angles(4 * lane, lane, lane_width)
    first = jnp.concatenate([cos_o, -sin_o], axis=0).astype(bf16)
    last = (jnp.concatenate([cos_o.T, -sin_o.T], axis=1) / (outer * lane_width)).astype(bf16)
    inner = jnp.block([[cos_i, -sin_i], [sin_i, cos_i]]).astype(bf16)
    inner_back = jnp.block([[cos_i, sin_i], [-sin_i, cos_i]]).astype(bf16)
    return first, last, inner, inner_back, cos_t, sin_t


def forward(signal, first, inner, cos_t, sin_t):
    outer = cos_t.shape[0]
    rows = []
    for at in range(0, len(signal), 2):
        pair = signal[at : at + 2]
        wide = jnp.dot(first, jnp.concatenate(pair, axis=1), preferred_element_type=f32)
        for i in range(len(pair)):
            part = wide[:, i * lane_width : (i + 1) * lane_width]
            real, imag = part[:outer], part[outer:]
            rows.append(
                jnp.concatenate(
                    [
                        (real * cos_t + imag * sin_t).astype(bf16),
                        (imag * cos_t - real * sin_t).astype(bf16),
                    ],
                    axis=1,
                )
            )
    return jnp.dot(jnp.concatenate(rows, axis=0), inner, preferred_element_type=f32)


def filter_kernel(first, inner, cos_t, sin_t, taps, spectrum):
    count, outer = taps.shape[0], taps.shape[1]
    signal = [taps[i].astype(bf16) for i in range(count)]
    out = forward(signal, first[...], inner[...], cos_t[...], sin_t[...])
    spectrum[...] = out.astype(bf16).reshape(count, outer, 2 * lane_width)


def convolve_block(tables, signal, filt):
    first, last, inner, inner_back, cos, sin = tables
    outer = cos.shape[0]
    sig = forward(signal, first, inner, cos, sin)
    filt = filt.astype(f32)
    sig_re, sig_im = sig[:, :lane_width], sig[:, lane_width:]
    filt_re, filt_im = filt[:, :lane_width], filt[:, lane_width:]
    prod = jnp.concatenate(
        [
            (filt_re * sig_re - filt_im * sig_im).astype(bf16),
            (filt_re * sig_im + filt_im * sig_re).astype(bf16),
        ],
        axis=1,
    )
    back = jnp.dot(prod, inner_back, preferred_element_type=f32)
    parts = []
    for at in range(0, len(signal), 2):
        cols = []
        for i in range(at, min(at + 2, len(signal))):
            rows = back[i * outer : (i + 1) * outer]
            real, imag = rows[:, :lane_width], rows[:, lane_width:]
            cols.append(
                jnp.concatenate(
                    [
                        (real * cos - imag * sin).astype(bf16),
                        (imag * cos + real * sin).astype(bf16),
                    ],
                    axis=0,
                )
            )
        wide = jnp.dot(last, jnp.concatenate(cols, axis=1), preferred_element_type=f32)
        for i in range(len(cols)):
            parts.append(wide[:, i * lane_width : (i + 1) * lane_width].astype(bf16))
    return parts


def conv_kernel(first, last, inner, inner_back, cos_t, sin_t, mixed, spectrum, conv):
    count, outer = mixed.shape[0], mixed.shape[1]
    tables = (first[...], last[...], inner[...], inner_back[...], cos_t[...], sin_t[...])
    filt = spectrum[...].reshape(count * outer, 2 * lane_width)
    parts = convolve_block(tables, [mixed[i] for i in range(count)], filt)
    for i in range(count):
        conv[i] = parts[i]


def whole(array):
    return pl.BlockSpec(array.shape, lambda i: (0,) * array.ndim)


def block_of(count):
    return max(b for b in range(1, 9) if count % b == 0)


def transform_filter(tables, taps):
    first, last, inner, inner_back, cos_t, sin_t = tables
    count, outer, lanes = taps.shape
    block = block_of(count)
    fixed = (first, inner, cos_t, sin_t)
    return pl.pallas_call(
        filter_kernel,
        grid=(count // block,),
        in_specs=[whole(a) for a in fixed] + [pl.BlockSpec((block, outer, lanes), lambda i: (i, 0, 0))],
        out_specs=pl.BlockSpec((block, outer, 2 * lanes), lambda i: (i, 0, 0)),
        out_shape=jax.ShapeDtypeStruct((count, outer, 2 * lanes), bf16),
        cost_estimate=pl.CostEstimate(
            flops=count * outer * lanes * 1536, bytes_accessed=count * outer * lanes * 8, transcendentals=0
        ),
        name="filter_transform",
    )(*fixed, taps)


def convolve(tables, mixed, spectrum):
    count, outer, lanes = mixed.shape
    block = block_of(count)
    return pl.pallas_call(
        conv_kernel,
        grid=(count // block,),
        in_specs=[whole(a) for a in tables]
        + [
            pl.BlockSpec((block, outer, lanes), lambda i: (i, 0, 0)),
            pl.BlockSpec((block, outer, 2 * lanes), lambda i: (i, 0, 0)),
        ],
        out_specs=pl.BlockSpec((block, outer, lanes), lambda i: (i, 0, 0)),
        out_shape=jax.ShapeDtypeStruct((count, outer, lanes), bf16),
        cost_estimate=pl.CostEstimate(
            flops=count * outer * lanes * 3072, bytes_accessed=count * outer * lanes * 8, transcendentals=0
        ),
        name="convolve",
    )(*tables, mixed, spectrum)


MESH = pl.DeviceIdType.MESH


def layer_kernel(
    first, last, inner, inner_back, cos_t, sin_t, key, value, gate, skip, kernel, weight,
    gathered, weights,
    taps, tall, wide, spectrum, mixed_out, mixed_in, conv_out, conv_in, gated,
    taps_sem, here_sem, w_send, w_recv, in_send, in_recv, out_send, out_recv, g_send, g_recv,
):
    segs, chunks, chans, tokens = key.shape
    groups = gathered.shape[0]
    share = gathered.shape[-1]
    outer = cos_t.shape[0]
    slabs = tokens // lane_width
    step = slabs + 8
    tall_step = outer + 8
    block = 8
    s = lax.axis_index("seg")
    h = lax.axis_index("ch")

    def seg_peer(d):
        return lax.rem(s + d, segs)

    def ch_peer(d):
        return lax.rem(h + d, groups)

    fetch = pltpu.make_async_copy(kernel.at[s], taps, taps_sem)
    fetch.start()
    barrier = pltpu.get_barrier_semaphore()
    for d in range(1, segs):
        pl.semaphore_signal(barrier, inc=1, device_id=(seg_peer(d), h), device_id_type=MESH)
    for d in range(1, groups):
        pl.semaphore_signal(barrier, inc=1, device_id=(s, ch_peer(d)), device_id_type=MESH)
    pl.semaphore_wait(barrier, segs + groups - 2)

    def lanes(j):
        return pl.ds(pl.multiple_of(j * lane_width, lane_width), lane_width)

    def send_in(k, d):
        return pltpu.make_async_remote_copy(
            src_ref=mixed_out.at[k, d], dst_ref=mixed_in.at[k, s],
            send_sem=in_send.at[k, d], recv_sem=in_recv.at[k, d],
            device_id=(seg_peer(d), h), device_id_type=MESH,
        )

    def send_out(k, d):
        return pltpu.make_async_remote_copy(
            src_ref=conv_out.at[k, seg_peer(d)], dst_ref=conv_in.at[k, s],
            send_sem=out_send.at[k, d], recv_sem=out_recv.at[k, d],
            device_id=(seg_peer(d), h), device_id_type=MESH,
        )

    def send_gated(k, d):
        peer = ch_peer(d)
        part = pl.ds(pl.multiple_of(peer * share, lane_width), share)
        return pltpu.make_async_remote_copy(
            src_ref=gated.at[k, :, :, part], dst_ref=gathered.at[h, :, k],
            send_sem=g_send.at[k, d], recv_sem=g_recv.at[k, d],
            device_id=(s, peer), device_id_type=MESH,
        )

    def send_weight(d):
        return pltpu.make_async_remote_copy(
            src_ref=weight, dst_ref=weights.at[h],
            send_sem=w_send.at[d], recv_sem=w_recv.at[d],
            device_id=(s, ch_peer(d)), device_id_type=MESH,
        )

    for k in range(chunks):
        for d in far_first(segs):
            peer = seg_peer(d)

            def mix(j, carry):
                both = key[peer, k, :, lanes(j)].astype(f32) * value[peer, k, :, lanes(j)].astype(f32)
                wide[pl.ds(j, chans, stride=step), :] = both
                return carry

            lax.fori_loop(0, slabs, mix, 0, unroll=4)
            into = mixed_out.at[k, d] if d else mixed_in.at[k, s]
            for i in range(chans):
                into[i] = wide[i * step : i * step + slabs, :].astype(bf16)
            if d:
                send_in(k, d).start()
        if k == 0:
            for d in range(1, groups):
                send_weight(d).start()
    own_weight = pltpu.make_async_copy(weight, weights.at[h], here_sem.at[chunks])
    own_weight.start()

    fetch.wait()
    for k in range(chunks):

        def spread(j, carry):
            tall[pl.ds(j, chans, stride=tall_step), :] = taps[k, :, lanes(j)]
            return carry

        lax.fori_loop(0, outer, spread, 0, unroll=4)
        for at in range(0, chans, block):
            signal = [
                tall[i * tall_step : i * tall_step + outer, :].astype(bf16)
                for i in range(at, at + block)
            ]
            out = forward(signal, first[...], inner[...], cos_t[...], sin_t[...])
            spectrum[k, at : at + block] = out.astype(bf16).reshape(block, outer, 2 * lane_width)

    for k in range(chunks):
        for d in range(1, segs):
            send_in(k, d).wait_recv()

        for at in range(0, chans, block):
            signal = [mixed_in[k, :, i].reshape(outer, lane_width) for i in range(at, at + block)]
            filt = spectrum[k, at : at + block].reshape(block * outer, 2 * lane_width)
            tables = (first[...], last[...], inner[...], inner_back[...], cos_t[...], sin_t[...])
            parts = convolve_block(tables, signal, filt)
            for i in range(block):
                conv_out[k, :, at + i] = parts[i].reshape(segs, slabs, lane_width)
        for d in far_first(segs):
            if d:
                send_out(k, d).start()

    own_gated = []
    for k in range(chunks):
        for d in range(segs):
            peer = seg_peer(d)
            if d:
                peer = lax.rem(s + segs - d, segs)
                send_out(k, d).wait_recv()
            source = conv_in.at[k, peer] if d else conv_out.at[k, s]
            for i in range(chans):
                wide[i * step : i * step + slabs, :] = source[i].astype(f32)
            gain = skip[peer, k]

            def combine(j, carry):
                conv = wide[pl.ds(j, chans, stride=step), :]
                both = key[peer, k, :, lanes(j)].astype(f32) * value[peer, k, :, lanes(j)].astype(f32)
                total = gate[peer, k, :, lanes(j)].astype(f32) * (conv + gain * both)
                gated[k, peer, :, lanes(j)] = total.astype(bf16)
                return carry

            lax.fori_loop(0, slabs, combine, 0, unroll=4)
        for d in range(1, groups):
            send_gated(k, d).start()
        part = pl.ds(pl.multiple_of(h * share, lane_width), share)
        own = pltpu.make_async_copy(gated.at[k, :, :, part], gathered.at[h, :, k], here_sem.at[k])
        own.start()
        own_gated.append(own)

    for d in range(1, groups):
        send_weight(d).wait()
    own_weight.wait()
    for k in range(chunks):
        for d in range(1, segs):
            send_in(k, d).wait_send()
            send_out(k, d).wait_send()
        for d in range(1, groups):
            send_gated(k, d).wait()
        own_gated[k].wait()


def far_first(segs):
    return [d for d in range(segs - 1, 0, -1)] + [0]


def whole_layer(gate_in, key_in, value_in, kernel, skip_gain, out_weight, chans):
    segs, groups = lax.axis_size("seg"), lax.axis_size("ch")
    channels, tokens = key_in.shape
    full_len = kernel.shape[1]
    outer = full_len // lane_width
    slabs = tokens // lane_width
    features = out_weight.shape[1]
    chunks = channels // segs // chans
    share = tokens // groups
    tables = make_tables(outer)
    split = (segs, chunks, chans)
    args = (
        *tables,
        key_in.reshape(*split, tokens),
        value_in.reshape(*split, tokens),
        gate_in.reshape(*split, tokens),
        skip_gain.reshape(*split, 1),
        kernel.reshape(*split, full_len),
        out_weight,
    )
    vmem = pl.BlockSpec(memory_space=pltpu.VMEM)
    hbm = pl.BlockSpec(memory_space=pl.ANY)
    piece = pltpu.VMEM((chunks, segs, chans, slabs, lane_width), bf16)
    dma = pltpu.SemaphoreType.DMA
    gathered, weights = pl.pallas_call(
        layer_kernel,
        in_specs=[vmem] * 10 + [hbm, vmem],
        out_specs=[hbm, hbm],
        out_shape=[
            jax.ShapeDtypeStruct((groups, segs, chunks, chans, share), bf16),
            jax.ShapeDtypeStruct((groups, channels, features), bf16),
        ],
        scratch_shapes=[
            pltpu.VMEM((chunks, chans, full_len), f32),
            pltpu.VMEM((chans * (outer + 8), lane_width), f32),
            pltpu.VMEM((chans * (slabs + 8), lane_width), f32),
            pltpu.VMEM((chunks, chans, outer, 2 * lane_width), bf16),
            piece, piece, piece, piece,
            pltpu.VMEM((chunks, segs, chans, tokens), bf16),
            dma, dma((chunks + 1,)),
            dma((groups,)), dma((groups,)),
            dma((chunks, segs)), dma((chunks, segs)), dma((chunks, segs)), dma((chunks, segs)),
            dma((chunks, groups)), dma((chunks, groups)),
        ],
        compiler_params=pltpu.CompilerParams(
            collective_id=0, has_side_effects=True, vmem_limit_bytes=56 * 1024 * 1024
        ),
        name="layer",
    )(*args)
    result = lax.dot_general(
        gathered.reshape(groups * channels, share),
        weights.reshape(groups * channels, features),
        (((0,), (0,)), ((), ())),
        preferred_element_type=f32,
    )
    return result.astype(bf16)


def on_device(gate_in, key_in, value_in, kernel, skip_gain, out_weight):
    seg_count = lax.axis_size("seg")
    seg_index = lax.axis_index("seg")
    channels, tokens = key_in.shape
    full_len = kernel.shape[1]
    outer = full_len // lane_width
    tables = make_tables(outer)
    col_count = channels // seg_count
    sublanes = 16
    if col_count % sublanes == 0 and tokens // lax.axis_size("ch") % lane_width == 0:
        return whole_layer(gate_in, key_in, value_in, kernel, skip_gain, out_weight, sublanes)
    mixed = key_in.astype(f32) * value_in.astype(f32)
    mixed_sent = mixed.astype(bf16).reshape(channels, tokens // lane_width, lane_width)
    col_mixed = lax.all_to_all(mixed_sent, "seg", split_axis=0, concat_axis=1, tiled=True)
    taps = lax.dynamic_slice_in_dim(kernel, seg_index * col_count, col_count, 0)
    spectrum = transform_filter(tables, taps.astype(bf16).reshape(col_count, outer, lane_width))
    col_conv = convolve(tables, col_mixed, spectrum)
    conv = lax.all_to_all(col_conv, "seg", split_axis=1, concat_axis=0, tiled=True)
    conv = conv.reshape(channels, tokens).astype(f32)
    gated = (gate_in.astype(f32) * (conv + skip_gain[:, None] * mixed)).astype(bf16)
    mine = lax.all_to_all(gated, "ch", split_axis=1, concat_axis=0, tiled=True)
    weight = lax.all_gather(out_weight, "ch", axis=0, tiled=True)
    result = lax.dot_general(
        mine, weight, (((0,), (0,)), ((), ())), preferred_element_type=f32
    )
    return result.astype(bf16)


def solution(mesh):
    placed = (P("ch", "seg"), P("ch", "seg"), P("ch", "seg"), P("ch", None), P("ch"), P("ch", None))
    return jax.shard_map(
        on_device, mesh=mesh, in_specs=placed, out_specs=P(("seg", "ch"), None), check_vma=False
    )
```

```python
import functools
import math

import jax
import jax.numpy as jnp
import numpy as np
from jax import lax
from jax.experimental import pallas as pl
from jax.experimental.pallas import tpu as pltpu
from jax.sharding import PartitionSpec as P

lane_width = 128
bf16 = jnp.bfloat16
f32 = jnp.float32


def angles(rows, cols, period):
    theta = (rows[:, None] * cols[None, :] % (4 * period)) * (2.0 * math.pi / (4 * period))
    return np.cos(theta), np.sin(theta)


def make_tables(outer):
    quarter = 4 * np.arange(outer) + 1
    row = np.arange(outer)
    lane = np.arange(lane_width)
    cos_o, sin_o = angles(quarter, row, outer)
    cos_t, sin_t = angles(quarter, lane, outer * lane_width)
    cos_i, sin_i = angles(4 * lane, lane, lane_width)
    first = np.concatenate([cos_o, -sin_o], axis=0)
    last = np.concatenate([cos_o.T, -sin_o.T], axis=1) / (outer * lane_width)
    inner = np.block([[cos_i, -sin_i], [sin_i, cos_i]])
    inner_back = np.block([[cos_i, sin_i], [-sin_i, cos_i]])
    narrow = [jnp.asarray(m.astype(np.float32).astype(bf16)) for m in (first, last, inner, inner_back)]
    return (*narrow, jnp.asarray(cos_t.astype(np.float32)), jnp.asarray(sin_t.astype(np.float32)))


def forward(signal, first, inner, cos_t, sin_t):
    outer = cos_t.shape[0]
    rows = []
    for at in range(0, len(signal), 2):
        pair = signal[at : at + 2]
        wide = jnp.dot(first, jnp.concatenate(pair, axis=1), preferred_element_type=f32)
        for i in range(len(pair)):
            part = wide[:, i * lane_width : (i + 1) * lane_width]
            real, imag = part[:outer], part[outer:]
            rows.append(
                jnp.concatenate(
                    [
                        (real * cos_t + imag * sin_t).astype(bf16),
                        (imag * cos_t - real * sin_t).astype(bf16),
                    ],
                    axis=1,
                )
            )
    return jnp.dot(jnp.concatenate(rows, axis=0), inner, preferred_element_type=f32)


def filter_kernel(first, inner, cos_t, sin_t, taps, spectrum):
    count, outer = taps.shape[0], taps.shape[1]
    signal = [taps[i].astype(bf16) for i in range(count)]
    out = forward(signal, first[...], inner[...], cos_t[...], sin_t[...])
    spectrum[...] = out.astype(bf16).reshape(count, outer, 2 * lane_width)


def convolve_block(tables, signal, filt):
    first, last, inner, inner_back, cos, sin = tables
    outer = cos.shape[0]
    sig = forward(signal, first, inner, cos, sin)
    filt = filt.astype(f32)
    sig_re, sig_im = sig[:, :lane_width], sig[:, lane_width:]
    filt_re, filt_im = filt[:, :lane_width], filt[:, lane_width:]
    prod = jnp.concatenate(
        [
            (filt_re * sig_re - filt_im * sig_im).astype(bf16),
            (filt_re * sig_im + filt_im * sig_re).astype(bf16),
        ],
        axis=1,
    )
    back = jnp.dot(prod, inner_back, preferred_element_type=f32)
    parts = []
    for at in range(0, len(signal), 2):
        cols = []
        for i in range(at, min(at + 2, len(signal))):
            rows = back[i * outer : (i + 1) * outer]
            real, imag = rows[:, :lane_width], rows[:, lane_width:]
            cols.append(
                jnp.concatenate(
                    [
                        (real * cos - imag * sin).astype(bf16),
                        (imag * cos + real * sin).astype(bf16),
                    ],
                    axis=0,
                )
            )
        wide = jnp.dot(last, jnp.concatenate(cols, axis=1), preferred_element_type=f32)
        for i in range(len(cols)):
            parts.append(wide[:, i * lane_width : (i + 1) * lane_width].astype(bf16))
    return parts


def conv_kernel(first, last, inner, inner_back, cos_t, sin_t, mixed, spectrum, conv):
    count, outer = mixed.shape[0], mixed.shape[1]
    tables = (first[...], last[...], inner[...], inner_back[...], cos_t[...], sin_t[...])
    filt = spectrum[...].reshape(count * outer, 2 * lane_width)
    parts = convolve_block(tables, [mixed[i] for i in range(count)], filt)
    for i in range(count):
        conv[i] = parts[i]


def whole(array):
    return pl.BlockSpec(array.shape, lambda i: (0,) * array.ndim)


def block_of(count):
    return max(b for b in range(1, 9) if count % b == 0)


def transform_filter(tables, taps):
    first, last, inner, inner_back, cos_t, sin_t = tables
    count, outer, lanes = taps.shape
    block = block_of(count)
    fixed = (first, inner, cos_t, sin_t)
    return pl.pallas_call(
        filter_kernel,
        grid=(count // block,),
        in_specs=[whole(a) for a in fixed] + [pl.BlockSpec((block, outer, lanes), lambda i: (i, 0, 0))],
        out_specs=pl.BlockSpec((block, outer, 2 * lanes), lambda i: (i, 0, 0)),
        out_shape=jax.ShapeDtypeStruct((count, outer, 2 * lanes), bf16),
        cost_estimate=pl.CostEstimate(
            flops=count * outer * lanes * 1536, bytes_accessed=count * outer * lanes * 8, transcendentals=0
        ),
        name="filter_transform",
    )(*fixed, taps)


def convolve(tables, mixed, spectrum):
    count, outer, lanes = mixed.shape
    block = block_of(count)
    return pl.pallas_call(
        conv_kernel,
        grid=(count // block,),
        in_specs=[whole(a) for a in tables]
        + [
            pl.BlockSpec((block, outer, lanes), lambda i: (i, 0, 0)),
            pl.BlockSpec((block, outer, 2 * lanes), lambda i: (i, 0, 0)),
        ],
        out_specs=pl.BlockSpec((block, outer, lanes), lambda i: (i, 0, 0)),
        out_shape=jax.ShapeDtypeStruct((count, outer, lanes), bf16),
        cost_estimate=pl.CostEstimate(
            flops=count * outer * lanes * 3072, bytes_accessed=count * outer * lanes * 8, transcendentals=0
        ),
        name="convolve",
    )(*tables, mixed, spectrum)


MESH = pl.DeviceIdType.MESH


def layer_kernel(
    first, last, inner, inner_back, cos_t, sin_t, key, value, gate, skip, kernel, weight,
    gathered, weights,
    gains, taps, tall, wide, spectrum, mixed_out, mixed_in, conv_out, conv_in, gated,
    taps_sem, here_sem, w_send, w_recv, in_send, in_recv, out_send, out_recv, g_send, g_recv,
):
    segs, chunks, chans, tokens = key.shape
    groups = gathered.shape[0]
    share = gathered.shape[-1]
    outer = cos_t.shape[0]
    slabs = tokens // lane_width
    step = slabs + 8
    tall_step = outer + 8
    block = 8
    s = lax.axis_index("seg")
    h = lax.axis_index("ch")

    def seg_peer(d):
        return lax.rem(s + d, segs)

    def ch_peer(d):
        return lax.rem(h + d, groups)

    fetch = pltpu.make_async_copy(kernel.at[s], taps, taps_sem)
    fetch.start()
    barrier = pltpu.get_barrier_semaphore()
    for d in range(1, segs):
        pl.semaphore_signal(barrier, inc=1, device_id=(seg_peer(d), h), device_id_type=MESH)
    for d in range(1, groups):
        pl.semaphore_signal(barrier, inc=1, device_id=(s, ch_peer(d)), device_id_type=MESH)
    pl.semaphore_wait(barrier, segs + groups - 2)

    def lanes(j):
        return pl.ds(pl.multiple_of(j * lane_width, lane_width), lane_width)

    def send_in(k, d):
        return pltpu.make_async_remote_copy(
            src_ref=mixed_out.at[k, d], dst_ref=mixed_in.at[k, s],
            send_sem=in_send.at[k, d], recv_sem=in_recv.at[k, d],
            device_id=(seg_peer(d), h), device_id_type=MESH,
        )

    def send_out(k, d):
        return pltpu.make_async_remote_copy(
            src_ref=conv_out.at[k, seg_peer(d)], dst_ref=conv_in.at[k, s],
            send_sem=out_send.at[k, d], recv_sem=out_recv.at[k, d],
            device_id=(seg_peer(d), h), device_id_type=MESH,
        )

    def send_gated(k, d):
        peer = ch_peer(d)
        part = pl.ds(pl.multiple_of(peer * share, lane_width), share)
        return pltpu.make_async_remote_copy(
            src_ref=gated.at[k, :, :, part], dst_ref=gathered.at[h, :, k],
            send_sem=g_send.at[k, d], recv_sem=g_recv.at[k, d],
            device_id=(s, peer), device_id_type=MESH,
        )

    def send_weight(d):
        return pltpu.make_async_remote_copy(
            src_ref=weight, dst_ref=weights.at[h],
            send_sem=w_send.at[d], recv_sem=w_recv.at[d],
            device_id=(s, ch_peer(d)), device_id_type=MESH,
        )

    for k in range(chunks):
        for d in far_first(segs):
            peer = seg_peer(d)

            def mix(j, carry):
                both = key[peer, k, :, lanes(j)].astype(f32) * value[peer, k, :, lanes(j)].astype(f32)
                wide[pl.ds(j, chans, stride=step), :] = both
                return carry

            lax.fori_loop(0, slabs, mix, 0, unroll=4)
            into = mixed_out.at[k, d] if d else mixed_in.at[k, s]
            for i in range(chans):
                into[i] = wide[i * step : i * step + slabs, :].astype(bf16)
            if d:
                send_in(k, d).start()
        if k == 0:
            for d in range(1, groups):
                send_weight(d).start()
    own_weight = pltpu.make_async_copy(weight, weights.at[h], here_sem.at[chunks])
    own_weight.start()

    for g in range(segs):
        for k in range(chunks):
            for i in range(chans):
                level = skip[(g * chunks + k) * chans + i]
                gains[g, k, i : i + 1, :] = jnp.full((1, lane_width), level, f32)

    fetch.wait()
    for k in range(chunks):

        def spread(j, carry):
            tall[pl.ds(j, chans, stride=tall_step), :] = taps[k, :, lanes(j)]
            return carry

        lax.fori_loop(0, outer, spread, 0, unroll=4)
        for at in range(0, chans, block):
            signal = [
                tall[i * tall_step : i * tall_step + outer, :].astype(bf16)
                for i in range(at, at + block)
            ]
            out = forward(signal, first[...], inner[...], cos_t[...], sin_t[...])
            spectrum[k, at : at + block] = out.astype(bf16).reshape(block, outer, 2 * lane_width)

    for k in range(chunks):
        for d in range(1, segs):
            send_in(k, d).wait_recv()

        for at in range(0, chans, block):
            signal = [mixed_in[k, :, i].reshape(outer, lane_width) for i in range(at, at + block)]
            filt = spectrum[k, at : at + block].reshape(block * outer, 2 * lane_width)
            tables = (first[...], last[...], inner[...], inner_back[...], cos_t[...], sin_t[...])
            parts = convolve_block(tables, signal, filt)
            for i in range(block):
                conv_out[k, :, at + i] = parts[i].reshape(segs, slabs, lane_width)
        for d in far_first(segs):
            if d:
                send_out(k, d).start()

    own_gated = []
    for k in range(chunks):
        for d in range(segs):
            peer = seg_peer(d)
            if d:
                peer = lax.rem(s + segs - d, segs)
                send_out(k, d).wait_recv()
            source = conv_in.at[k, peer] if d else conv_out.at[k, s]
            for i in range(chans):
                wide[i * step : i * step + slabs, :] = source[i].astype(f32)
            gain = gains[peer, k]

            def combine(j, carry):
                conv = wide[pl.ds(j, chans, stride=step), :]
                both = key[peer, k, :, lanes(j)].astype(f32) * value[peer, k, :, lanes(j)].astype(f32)
                total = gate[peer, k, :, lanes(j)].astype(f32) * (conv + gain * both)
                gated[k, peer, :, lanes(j)] = total.astype(bf16)
                return carry

            lax.fori_loop(0, slabs, combine, 0, unroll=4)
        for d in range(1, groups):
            send_gated(k, d).start()
        part = pl.ds(pl.multiple_of(h * share, lane_width), share)
        own = pltpu.make_async_copy(gated.at[k, :, :, part], gathered.at[h, :, k], here_sem.at[k])
        own.start()
        own_gated.append(own)

    for d in range(1, groups):
        send_weight(d).wait()
    own_weight.wait()
    for k in range(chunks):
        for d in range(1, segs):
            send_in(k, d).wait_send()
            send_out(k, d).wait_send()
        for d in range(1, groups):
            send_gated(k, d).wait()
        own_gated[k].wait()


def far_first(segs):
    return [d for d in range(segs - 1, 0, -1)] + [0]


def whole_layer(gate_in, key_in, value_in, kernel, skip_gain, out_weight, chans):
    segs, groups = lax.axis_size("seg"), lax.axis_size("ch")
    channels, tokens = key_in.shape
    full_len = kernel.shape[1]
    outer = full_len // lane_width
    slabs = tokens // lane_width
    features = out_weight.shape[1]
    chunks = channels // segs // chans
    share = tokens // groups
    tables = make_tables(outer)
    split = (segs, chunks, chans)
    args = (
        *tables,
        key_in.reshape(*split, tokens),
        value_in.reshape(*split, tokens),
        gate_in.reshape(*split, tokens),
        skip_gain,
        kernel.reshape(*split, full_len),
        out_weight,
    )
    vmem = pl.BlockSpec(memory_space=pltpu.VMEM)
    hbm = pl.BlockSpec(memory_space=pl.ANY)
    piece = pltpu.VMEM((chunks, segs, chans, slabs, lane_width), bf16)
    dma = pltpu.SemaphoreType.DMA
    gathered, weights = pl.pallas_call(
        layer_kernel,
        in_specs=[vmem] * 9 + [pl.BlockSpec(memory_space=pltpu.SMEM), hbm, vmem],
        out_specs=[hbm, hbm],
        out_shape=[
            jax.ShapeDtypeStruct((groups, segs, chunks, chans, share), bf16),
            jax.ShapeDtypeStruct((groups, channels, features), bf16),
        ],
        scratch_shapes=[
            pltpu.VMEM((segs, chunks, chans, lane_width), f32),
            pltpu.VMEM((chunks, chans, full_len), f32),
            pltpu.VMEM((chans * (outer + 8), lane_width), f32),
            pltpu.VMEM((chans * (slabs + 8), lane_width), f32),
            pltpu.VMEM((chunks, chans, outer, 2 * lane_width), bf16),
            piece, piece, piece, piece,
            pltpu.VMEM((chunks, segs, chans, tokens), bf16),
            dma, dma((chunks + 1,)),
            dma((groups,)), dma((groups,)),
            dma((chunks, segs)), dma((chunks, segs)), dma((chunks, segs)), dma((chunks, segs)),
            dma((chunks, groups)), dma((chunks, groups)),
        ],
        compiler_params=pltpu.CompilerParams(
            collective_id=0, has_side_effects=True, vmem_limit_bytes=56 * 1024 * 1024
        ),
        name="layer",
    )(*args)
    result = lax.dot_general(
        gathered.reshape(groups * channels, share),
        weights.reshape(groups * channels, features),
        (((0,), (0,)), ((), ())),
        preferred_element_type=f32,
    )
    return result.astype(bf16)


def on_device(gate_in, key_in, value_in, kernel, skip_gain, out_weight):
    seg_count = lax.axis_size("seg")
    seg_index = lax.axis_index("seg")
    channels, tokens = key_in.shape
    full_len = kernel.shape[1]
    outer = full_len // lane_width
    tables = make_tables(outer)
    col_count = channels // seg_count
    sublanes = 8
    if col_count % sublanes == 0 and tokens // lax.axis_size("ch") % lane_width == 0:
        return whole_layer(gate_in, key_in, value_in, kernel, skip_gain, out_weight, sublanes)
    mixed = key_in.astype(f32) * value_in.astype(f32)
    mixed_sent = mixed.astype(bf16).reshape(channels, tokens // lane_width, lane_width)
    col_mixed = lax.all_to_all(mixed_sent, "seg", split_axis=0, concat_axis=1, tiled=True)
    taps = lax.dynamic_slice_in_dim(kernel, seg_index * col_count, col_count, 0)
    spectrum = transform_filter(tables, taps.astype(bf16).reshape(col_count, outer, lane_width))
    col_conv = convolve(tables, col_mixed, spectrum)
    conv = lax.all_to_all(col_conv, "seg", split_axis=1, concat_axis=0, tiled=True)
    conv = conv.reshape(channels, tokens).astype(f32)
    gated = (gate_in.astype(f32) * (conv + skip_gain[:, None] * mixed)).astype(bf16)
    mine = lax.all_to_all(gated, "ch", split_axis=1, concat_axis=0, tiled=True)
    weight = lax.all_gather(out_weight, "ch", axis=0, tiled=True)
    result = lax.dot_general(
        mine, weight, (((0,), (0,)), ((), ())), preferred_element_type=f32
    )
    return result.astype(bf16)


def solution(mesh):
    placed = (P("ch", "seg"), P("ch", "seg"), P("ch", "seg"), P("ch", None), P("ch"), P("ch", None))
    return jax.shard_map(
        on_device, mesh=mesh, in_specs=placed, out_specs=P(("seg", "ch"), None), check_vma=False
    )
```
